32 devices in a mesh: expert: 8 (over z, x), tensor: 4 (over y, core).
Axes of the slice: x: 2, y: 2, z: 4, core: 2. Of those that a mesh axis runs over, the one named last changes fastest.
Arguments:
- tokens: bfloat16 [1024, 4096], P('expert'), may hold values from -6 to 6
- scores: float32 [1024, 8], P('expert'), may hold values from -6 to 6
- expert_ids: int32 [1024, 8], P('expert'), may hold values from 0 to 31, all different within a row; in each aligned block of 128 rows (0 to 127, 128 to 255, ...) at most 64 rows name the same one
- gate_weight: bfloat16 [32, 1536, 4096], P('expert', 'tensor'), may hold values from -0.09375 to 0.09375
- up_weight: bfloat16 [32, 1536, 4096], P('expert', 'tensor'), may hold values from -0.09375 to 0.09375
- down_weight: bfloat16 [32, 1536, 4096], P('expert', 'tensor'), may hold values from -0.15625 to 0.15625
Outputs:
- mixed: bfloat16 [1024, 4096], P('expert', 'tensor')
The draws below stay inside these ranges and needn't reach their ends.
Inputs may be any that keep to these rules, and one draw needn't show every extreme that they name: `expert_ids`: each row names 8 different experts. Among the 128 rows of one owner (rows o * 128 to (o + 1) * 128 - 1) no expert is named more than 64 times.
All inputs are finite; a program needn't handle non-finite values.
Results may differ from the reference program's by a relative error of at most 0.018.
Values may be sent and summed in bfloat16 or wider, within the bound.
No kernel may reach another device: no remote copies, remote signals or barrier semaphores. Data moves between devices by JAX's collectives and lax.ppermute only.
A program may use at most 128 MiB of HBM per device.

```python
import math
import jax
import jax.numpy as jnp
import numpy as np
from jax import lax

D = 4096
FF = 1536
TOP = 8
EXP_DEV = 4
TOK_DEV = 128
EXPERTS = 32
TOKENS = 1024
M = 64
N_EXPERT = 8
N_TENSOR = 4


def block_scale(key, extent, shards, least, top_value):
    gain = 1.0
    for dim, shards_of in shards:
        heights = jax.random.uniform(jax.random.fold_in(jax.random.fold_in(key, 6), dim), (shards_of,), jnp.float32, least / len(shards), top_value / len(shards))
        gain = gain * jnp.repeat(jnp.exp(heights), extent[dim] // shards_of).reshape((-1,) + (1,) * (len(extent) - 1 - dim))
    return gain


def assign_block(key, own, number, rows, amount, top, bound, skew):
    sequence = jax.random.permutation(key, amount)
    heavy_load, ordinary = load_shares(amount, rows * top, bound, skew, True), load_shares(amount, rows * top, bound, skew, False)
    places = jnp.arange(amount)

    def named(tallies, rotation):
        used = int((tallies > 0).sum())
        fixed = max(1, used // 4)
        moved = fixed + (places - fixed + rotation * (used - fixed)) % max(1, amount - fixed)
        return jnp.zeros((amount,), jnp.int32).at[sequence[jnp.where(places < fixed, places, moved)]].set(jnp.asarray(tallies, jnp.int32))

    tallies = jnp.where(number % 4 == 0, named(heavy_load, number // 4), named(ordinary, number - number // 4 - 1))
    mixed = jax.random.permutation(jax.random.fold_in(own, 3), amount)
    source_of, taker = mixed[0:amount // 2 * 2:2], mixed[1:amount // 2 * 2:2]
    margin = jnp.minimum(tallies[source_of] - 1, bound - tallies[taker]) // 2
    margin = jnp.where((source_of == sequence[0]) | (taker == sequence[0]) | (tallies[taker] == 0), 0, jnp.maximum(margin, 0))
    moved = jax.random.randint(jax.random.fold_in(own, 4), (amount // 2,), 0, 1 << 20) % (margin + 1)
    tallies = tallies.at[source_of].add(-moved).at[taker].add(moved)
    items = jnp.searchsorted(jnp.cumsum(tallies), jnp.arange(rows * top), side="right").astype(jnp.int32)
    listing = items.reshape(top, rows).T
    listing = listing[jax.random.permutation(jax.random.fold_in(own, 1), rows)]
    rotation = jax.random.randint(jax.random.fold_in(own, 2), (rows, 1), 0, top)
    return jnp.take_along_axis(listing, (jnp.arange(top)[None, :] + rotation) % top, axis=1)


def load_shares(amount, total, most, slope, full):
    weights = [(1 << 20) // math.isqrt(standing ** slope) + 1 for standing in range(1, amount + 1)]
    largest = most if full else min(most, max(-(-total // amount), total * weights[0] // sum(weights)))
    least = 1 if total - largest >= amount - 1 else 0
    given, spare = [largest] + [least] * (amount - 1), total - largest - least * (amount - 1)
    while spare > 0:
        candidates = [i for i in range(1, amount) if given[i] < largest] or [i for i in range(1, amount) if given[i] < most]
        pool, left = sum([weights[i] for i in candidates]), spare
        for i in candidates:
            extra = min(most - given[i], max(1, left * weights[i] // pool), spare)
            given[i] = given[i] + extra
            spare = spare - extra
    return np.array(given)


def scatter_about(key, dims, deviation, bound, shards=(), kind=jnp.bfloat16):
    values = jax.random.normal(key, dims, jnp.float32) * deviation
    if len(shards) > 0:
        values = block_scale(key, dims, shards, -0.22, 0.18) * values
    return jnp.clip(values, min=-bound, max=bound).astype(kind)


def setup_inputs(seed: int = 0) -> dict:
    seeds = jax.random.split(jax.random.key(seed), 7)
    tokens = scatter_about(seeds[0], (TOKENS, D), 1.0, 6.0, ((0, 8),))
    scores = scatter_about(seeds[1], (TOKENS, TOP), 1.0, 6.0, ((0, 8),), jnp.float32)
    expert_ids_keys = jax.random.split(jax.random.fold_in(seeds[2], 1), TOKENS // TOK_DEV)
    expert_ids_turns = jax.random.permutation(jax.random.fold_in(seeds[2], 3), TOKENS // TOK_DEV)
    expert_ids = jax.vmap(lambda own, number: assign_block(jax.random.fold_in(seeds[2], 2), own, number, TOK_DEV, EXPERTS, TOP, M, 1))(expert_ids_keys, expert_ids_turns).reshape((TOKENS, TOP))
    gate_weight = scatter_about(seeds[3], (EXPERTS, FF, D), D ** -0.5, 0.09375, ((0, 8), (1, 4)))
    up_weight = scatter_about(seeds[4], (EXPERTS, FF, D), D ** -0.5, 0.09375, ((0, 8), (1, 4)))
    down_weight = scatter_about(seeds[5], (EXPERTS, FF, D), FF ** -0.5, 0.15625, ((0, 8), (1, 4)))
    return {"tokens": tokens, "scores": scores, "expert_ids": expert_ids, "gate_weight": gate_weight, "up_weight": up_weight, "down_weight": down_weight}


def gate_of(scores):
    lifted = jnp.exp(scores.astype(jnp.float32))
    return (lifted / jnp.sum(lifted, axis=-1, keepdims=True)).astype(jnp.bfloat16)


def slot_tables(expert_ids, gate_values, experts, blocks, capacity):
    rows_all = expert_ids.shape[0]
    block_rows = rows_all // blocks
    expert_count = experts.shape[0]
    matches = expert_ids[:, :, None] == experts[None, None, :]
    routed = jnp.any(matches, axis=1).astype(jnp.int32)
    chosen_gate = jnp.sum(jnp.where(matches, gate_values.astype(jnp.float32)[:, :, None], jnp.float32(0.0)), axis=1)
    folded = routed.reshape(blocks, block_rows, expert_count)
    rank_in_block = (jnp.cumsum(folded, axis=1) - folded).astype(jnp.int32)
    block_start = (jnp.arange(blocks, dtype=jnp.int32) * capacity)[:, None, None]
    slot_index = (block_start + rank_in_block).reshape(rows_all, expert_count).astype(jnp.int32)
    slot_index = jnp.where(routed == 1, slot_index, blocks * capacity).astype(jnp.int32)
    columns = jnp.broadcast_to(jnp.arange(expert_count, dtype=jnp.int32)[None, :], slot_index.shape)
    position = jnp.broadcast_to(jnp.arange(rows_all, dtype=jnp.int32)[:, None], slot_index.shape)
    slot_token = jnp.full((expert_count, blocks * capacity), rows_all, jnp.int32).at[columns, slot_index].set(position, mode="drop")
    slot_gate = jnp.zeros((expert_count, blocks * capacity), jnp.float32).at[columns, slot_index].set(chosen_gate, mode="drop")
    return slot_token, slot_gate


def reference(tokens, scores, expert_ids, gate_weight, up_weight, down_weight):
    gate_values = gate_of(scores)
    experts = jnp.arange(EXP_DEV * N_EXPERT, dtype=jnp.int32)
    slot_token, slot_gate = slot_tables(expert_ids, gate_values, experts, N_EXPERT, M)
    share = FF // N_TENSOR

    def one_expert(total, inputs):
        token_index, gate_column, w_gate, w_up, w_down = inputs
        rows = jnp.take(tokens, token_index, axis=0, mode="fill", fill_value=0)
        gate = jnp.dot(rows, w_gate.T, preferred_element_type=jnp.float32)
        upward = jnp.dot(rows, w_up.T, preferred_element_type=jnp.float32)
        hidden = (jax.nn.silu(gate) * upward).astype(jnp.bfloat16)
        pieces = hidden.reshape(hidden.shape[0], N_TENSOR, share).astype(jnp.float32)
        blocks_down = w_down.reshape(N_TENSOR, share, D).astype(jnp.float32)
        partial_value = jnp.einsum("cnf,nfd->ncd", pieces, blocks_down).astype(jnp.bfloat16)
        summed = jnp.sum(partial_value.astype(jnp.float32), axis=0)
        gated = summed * gate_column[:, None]
        total = total.at[token_index].add(gated, mode="drop")
        return total, jnp.float32(0.0)

    start = jnp.zeros((tokens.shape[0], D), jnp.float32)
    total = lax.scan(one_expert, start, (slot_token, slot_gate, gate_weight, up_weight, down_weight))[0]
    return total.astype(jnp.bfloat16)
```

```python
import functools

import jax
import jax.numpy as jnp
from jax import lax
from jax.experimental import pallas as pl
from jax.experimental.pallas import tpu as pltpu
from jax.sharding import PartitionSpec as P

TOP = 8
F32 = jnp.float32
BF16 = jnp.bfloat16


def tables_body(order, gates, pick, mix, *, owners, held, room):
    rows = gates.shape[-1]
    table = jnp.concatenate([gates[order[o]] for o in range(owners)], axis=0)
    routed = table > 0
    before = lax.broadcasted_iota(jnp.int32, (rows, rows), 0) < lax.broadcasted_iota(
        jnp.int32, (rows, rows), 1
    )
    rank = jnp.dot(routed.astype(BF16), before.astype(BF16), preferred_element_type=F32)
    rank = jnp.where(routed, rank, F32(-1.0)).astype(jnp.int32)
    slot = lax.broadcasted_iota(jnp.int32, (room, rows), 0)
    for o in range(owners):
        chosen, gated = [], []
        for e in range(held):
            i = o * held + e
            hit = rank[i : i + 1] == slot
            chosen.append(jnp.where(hit, F32(1.0), F32(0.0)))
            gated.append(jnp.where(hit, table[i : i + 1], F32(0.0)))
        pick[o] = jnp.concatenate(chosen, axis=0).astype(BF16)
        mix[o] = jnp.concatenate(gated, axis=0).T.astype(BF16)


def rise_body(where, *refs, quarters, owners, held, room, steps, start, last):
    pieces = refs[: quarters * (owners - 1)]
    rest = list(refs[quarters * (owners - 1) :])
    tokens, pick, gate_w, up_w = rest[:4]
    rest = rest[4:]
    begin = None if start else rest.pop(0)
    out = rest.pop(0)
    rows = rest.pop(0)
    total = rest.pop(0) if last else out
    j = pl.program_id(0)

    for q in range(quarters):

        @pl.when(j // steps == q)
        def _(q=q):
            for o in range(owners):
                source = tokens if o == 0 else pieces[q * (owners - 1) + o - 1]
                taken = jnp.dot(pick[o], source[...], preferred_element_type=F32).astype(BF16)
                for e in range(held):
                    rows[e, o * room : (o + 1) * room] = taken[e * room : (e + 1) * room]

    units = gate_w.shape[1]
    across = (((1,), (1,)), ((), ()))
    for e in range(held):
        new = jnp.concatenate(
            [
                lax.dot_general(rows[e], w[e], across, preferred_element_type=F32)
                for w in (gate_w, up_w)
            ],
            axis=1,
        )

        @pl.when(j == 0)
        def _(e=e, new=new):
            total[e] = new if begin is None else begin[e] + new

        @pl.when(j > 0)
        def _(e=e, new=new):
            total[e] += new

    if last:

        @pl.when(j == pl.num_programs(0) - 1)
        def _():
            for e in range(held):
                gate = total[e, :, :units]
                out[e] = (gate / (1.0 + jnp.exp(-gate)) * total[e, :, units:]).astype(BF16)


def fall_body(where, *refs, owners, held, room, received, split):
    hidden, mix, down_w = refs[:3]
    more = refs[3] if received else None
    outs = refs[3 + received : -1]
    part = refs[-1]
    for e in range(held):
        made = jnp.dot(hidden[e], down_w[e], preferred_element_type=F32).astype(BF16)
        for o in range(owners):
            part[o, e * room : (e + 1) * room] = made[o * room : (o + 1) * room]
    for o in range(owners):
        value = jnp.dot(mix[o], part[o], preferred_element_type=F32)
        if received:
            value = value + more[0, o].astype(F32)
        if split:
            outs[o][...] = value.astype(BF16)
        else:
            outs[0][0, o] = value.astype(BF16)


def fixed(shape):
    return pl.BlockSpec(shape, lambda j, s: (0,) * len(shape))


def local(tokens, scores, expert_ids, gate_weight, up_weight, down_weight):
    groups = lax.axis_size("expert")
    ranks = lax.axis_size("tensor")
    held, units, width = gate_weight.shape
    owner_rows = tokens.shape[0]
    share = width // ranks
    room = 2 * owner_rows * TOP // (held * groups)
    cores = 2
    ny = ranks // cores
    nx = ny if groups % ny == 0 else 1
    nz = groups // nx
    owners = groups
    chunk = min(512, share)
    steps = share // chunk
    slots = owners * room

    def along(axis, where_to, size):
        pairs = [(i, where_to(i)) for i in range(size)]
        return lambda v: lax.ppermute(v, axis, pairs)

    z_next = along("expert", lambda i: (i // nx + 1) % nz * nx + i % nx, groups)
    x_next = along("expert", lambda i: i // nx * nx + (i % nx + 1) % nx, groups)
    y_next = along("tensor", lambda k: (k // cores + 1) % ny * cores + k % cores, ranks)
    core_swap = along("tensor", lambda k: k ^ 1, ranks)

    def ring_gather(piece, nxt, n):
        got = [piece] * n
        for t in range(1, n):
            piece = nxt(piece)
            got[n - t] = piece
        return got

    def add(*values):
        return sum(v.astype(F32) for v in values).astype(BF16)

    def ring_reduce(parts, nxt):
        n = len(parts)
        total = add(*parts[n - 1])
        for t in range(1, n):
            moved = nxt(total)
            if n - 1 - t == 0:
                return (moved, *parts[0])
            total = add(moved, *parts[n - 1 - t])
        return parts[0]

    here = lax.axis_index("expert")
    rank = lax.axis_index("tensor")
    z, x, y, core = here // nx, here % nx, rank // cores, rank % cores

    def rank_at(yr, cr):
        return (y + yr) % ny * cores + (core + cr) % cores

    lifted = jnp.exp(scores)
    gate_values = (lifted / jnp.sum(lifted, axis=-1, keepdims=True)).astype(BF16)
    names = jnp.arange(groups * held, dtype=jnp.int32)
    dense = jnp.sum(
        jnp.where(
            expert_ids.T[:, None, :] == names[None, :, None],
            gate_values.T.astype(F32)[:, None, :],
            F32(0.0),
        ),
        axis=0,
    )

    narrow = lax.dynamic_slice_in_dim(tokens, rank * share, share, 1)
    lines = ring_gather(narrow, z_next, nz)
    mine = []
    for zr in range(nz):
        mine += ring_gather(lines[zr], x_next, nx)
    by_y = [ring_gather(p, y_next, ny) for p in mine[1:]]
    pieces = {}
    for yr in range(ny):
        pieces[yr, 0] = [p[yr] for p in by_y]
        pieces[yr, 1] = [core_swap(p[yr]) for p in by_y]

    gates = lax.all_to_all(
        dense.reshape(groups, held, owner_rows), "expert", split_axis=0, concat_axis=0, tiled=True
    )
    order = jnp.stack(
        [(z + zr) % nz * nx + (x + xr) % nx for zr in range(nz) for xr in range(nx)]
    ).astype(jnp.int32)
    pick, mix = pl.pallas_call(
        functools.partial(tables_body, owners=owners, held=held, room=room),
        grid_spec=pltpu.PrefetchScalarGridSpec(
            num_scalar_prefetch=1,
            grid=(1,),
            in_specs=[fixed(gates.shape)],
            out_specs=[
                fixed((owners, held * room, owner_rows)),
                fixed((owners, owner_rows, held * room)),
            ],
        ),
        out_shape=[
            jax.ShapeDtypeStruct((owners, held * room, owner_rows), BF16),
            jax.ShapeDtypeStruct((owners, owner_rows, held * room), BF16),
        ],
        name="tables",
    )(order, gates)

    def rise(quarters, begin, last, name):
        n = len(quarters)
        where = jnp.stack([rank_at(*q) for q in quarters]).astype(jnp.int32)
        given = [p for q in quarters for p in pieces[q]]

        def piece_spec(q):
            return pl.BlockSpec(
                (owner_rows, chunk), lambda j, s: (0, jnp.clip(j - q * steps, 0, steps - 1))
            )

        def column(j, s):
            return s[j // steps] * steps + j % steps

        weight = pl.BlockSpec((held, units, chunk), lambda j, s: (0, 0, column(j, s)))
        in_specs = [piece_spec(q) for q in range(n) for _ in range(owners - 1)]
        in_specs += [
            pl.BlockSpec((owner_rows, chunk), lambda j, s: (0, column(j, s))),
            fixed(pick.shape),
            weight,
            weight,
        ]
        given += [tokens, pick, gate_weight, up_weight]
        total = (held, slots, 2 * units)
        if begin is not None:
            in_specs.append(fixed(total))
            given.append(begin)
        scratch = [pltpu.VMEM((held, slots, chunk), BF16)]
        if last:
            scratch.append(pltpu.VMEM(total, F32))
        made = (held, slots, units) if last else total
        return pl.pallas_call(
            functools.partial(
                rise_body,
                quarters=n,
                owners=owners,
                held=held,
                room=room,
                steps=steps,
                start=begin is None,
                last=last,
            ),
            grid_spec=pltpu.PrefetchScalarGridSpec(
                num_scalar_prefetch=1,
                grid=(n * steps,),
                in_specs=in_specs,
                out_specs=fixed(made),
                scratch_shapes=scratch,
            ),
            out_shape=jax.ShapeDtypeStruct(made, BF16 if last else F32),
            cost_estimate=pl.CostEstimate(
                flops=n * share * slots * held * units * 4,
                bytes_accessed=n * share * held * units * 4,
                transcendentals=0,
            ),
            name=name,
        )(where, *given)

    sofar = rise([(0, 0), (0, 1)], None, False, "rise_near")
    hidden = rise([(yr, cr) for yr in range(1, ny) for cr in range(2)], sofar, True, "rise_far")

    def fall(quarters, received, split, name):
        n = len(quarters)
        where = jnp.stack([rank_at(*q) for q in quarters]).astype(jnp.int32)
        weight = pl.BlockSpec(
            (held, units, chunk), lambda j, s: (0, 0, s[j // steps] * steps + j % steps)
        )
        whole = pl.BlockSpec(
            (1, owners, owner_rows, chunk), lambda j, s: (j // steps, 0, 0, j % steps)
        )
        in_specs = [fixed(hidden.shape), fixed(mix.shape), weight]
        given = [hidden, mix, down_weight]
        if received is not None:
            in_specs.append(whole)
            given.append(received)
        if split:
            piece = pl.BlockSpec((owner_rows, chunk), lambda j, s: (0, j))
            out_specs = [piece] * owners
            out_shape = [jax.ShapeDtypeStruct((owner_rows, share), BF16)] * owners
        else:
            out_specs = [whole]
            out_shape = [jax.ShapeDtypeStruct((n, owners, owner_rows, share), BF16)]
        return pl.pallas_call(
            functools.partial(
                fall_body,
                owners=owners,
                held=held,
                room=room,
                received=received is not None,
                split=split,
            ),
            grid_spec=pltpu.PrefetchScalarGridSpec(
                num_scalar_prefetch=1,
                grid=(n * steps,),
                in_specs=in_specs,
                out_specs=out_specs,
                scratch_shapes=[pltpu.VMEM((owners, held * room, chunk), BF16)],
            ),
            out_shape=out_shape,
            cost_estimate=pl.CostEstimate(
                flops=n * share * slots * held * (units + owner_rows) * 2,
                bytes_accessed=n * share * held * units * 2,
                transcendentals=0,
            ),
            name=name,
        )(where, *given)

    parts = {}
    for yr in list(range(1, ny)) + [0]:
        away = fall([(yr, 1)], None, False, f"fall_away_{yr}")[0]
        parts[yr] = core_swap(away)
    kept = {yr: fall([(yr, 0)], parts[yr], True, f"fall_keep_{yr}") for yr in list(range(1, ny)) + [0]}

    def y_total(o):
        return ring_reduce([(kept[yr][o],) for yr in range(ny)], y_next)

    lines = []
    for zr in range(nz):
        lines.append(ring_reduce([y_total(zr * nx + xr) for xr in range(nx)], x_next))
    return add(*ring_reduce(lines, z_next))


def solution(mesh):
    in_specs = (
        P("expert", None),
        P("expert", None),
        P("expert", None),
        P("expert", "tensor", None),
        P("expert", "tensor", None),
        P("expert", "tensor", None),
    )
    out_specs = P("expert", "tensor")
    return jax.shard_map(local, mesh=mesh, in_specs=in_specs, out_specs=out_specs, check_vma=False)
```
